32 devices in a mesh: cuts: 4 (over y, x), space: 8 (over z, core).
Axes of the slice: x: 2, y: 2, z: 4, core: 2. Of those that a mesh axis runs over, the one named last changes fastest.
Arguments:
- starts: float32 [4, 3, 32, 64, 128], P('cuts', None, 'space'), may hold values from -3 to 3
Outputs:
- new_starts: float32 [4, 3, 32, 64, 128], P('cuts', None, 'space')
The draws below stay inside these ranges and needn't reach their ends.
All inputs are finite; a program needn't handle non-finite values.
Results may differ from the reference program's by a relative error of at most 0.0001.
Values sent between devices are 32-bit elements; how exact they have to be, the bound alone decides.
A program may use at most 64 MiB of HBM per device.

```python
import jax
import jax.numpy as jnp
from jax import lax

NY = 64
NZ = 128
FSTEPS = 16
CSTEPS = 2
SLICES = 4
NX = 32


def steps_of(stream_key, shape, cuts, least, largest):
    loudness, own = 1.0, jax.random.fold_in(stream_key, 6)
    for axis_at, shards_of in cuts:
        draws = jnp.exp(jax.random.uniform(jax.random.fold_in(own, axis_at), (shards_of,), jnp.float32, least / len(cuts), largest / len(cuts)))
        loudness = loudness * jnp.repeat(draws, shape[axis_at] // shards_of).reshape([-1 if axis == axis_at else 1 for axis in range(len(shape))])
    return loudness


def gaussian(key, extent, scale, bound, cuts=(), kind=jnp.bfloat16):
    gain = steps_of(key, extent, cuts, -0.22, 0.18) if cuts else 1.0
    result = jax.random.normal(key, extent, jnp.float32) * scale * gain
    return jnp.minimum(jnp.maximum(result, -bound), bound).astype(kind)


def setup_inputs(seed: int = 0) -> dict:
    key_of = jax.random.split(jax.random.key(seed), 2)
    starts = gaussian(key_of[0], (SLICES, 3, NX, NY, NZ), 0.5, 3.0, ((0, 4), (2, 8)), jnp.float32)
    return {"starts": starts}


fine_rate = 0.08
fine_advect = 0.04
coarse_rate = 0.16
coarse_advect = 0.16


def advance(extended, rate, advect):
    padded = jnp.pad(extended, ((0, 0), (0, 0), (1, 1), (1, 1)))
    centre = padded[:, 1:-1, 1:-1, 1:-1]
    x_plus = padded[:, 2:, 1:-1, 1:-1]
    x_minus = padded[:, :-2, 1:-1, 1:-1]
    y_plus = padded[:, 1:-1, 2:, 1:-1]
    y_minus = padded[:, 1:-1, :-2, 1:-1]
    z_plus = padded[:, 1:-1, 1:-1, 2:]
    z_minus = padded[:, 1:-1, 1:-1, :-2]
    laplace = (x_plus + x_minus) + (y_plus + y_minus) + (z_plus + z_minus) - 6.0 * centre
    convect = centre[0:1] * (x_plus - x_minus) + centre[1:2] * (y_plus - y_minus) + centre[2:3] * (z_plus - z_minus)
    return centre + rate * laplace - advect * convect


def one_step(field, rate, advect):
    return advance(jnp.pad(field, ((0, 0), (1, 1), (0, 0), (0, 0))), rate, advect)


def fine_whole(field):
    return lax.fori_loop(0, FSTEPS, lambda index, state: one_step(state, fine_rate, fine_advect), field)


def coarse_whole(field):
    return lax.fori_loop(0, CSTEPS, lambda index, state: one_step(state, coarse_rate, coarse_advect), field)


def restrict(field):
    blocks = field.reshape(field.shape[0], field.shape[1] // 2, 2, field.shape[2] // 2, 2, field.shape[3] // 2, 2)
    return jnp.sum(blocks, axis=(2, 4, 6)) * 0.125


def prolong(field):
    return jnp.repeat(jnp.repeat(jnp.repeat(field, 2, axis=1), 2, axis=2), 2, axis=3)


def reference(starts):
    ends = lax.map(fine_whole, starts)
    old_coarse = lax.map(lambda field: coarse_whole(restrict(field)), starts)
    change = ends - lax.map(prolong, old_coarse)

    def sweep(state, previous):
        advanced = coarse_whole(state)
        corrected = prolong(advanced) + previous
        return advanced + restrict(previous), corrected

    unused, corrected = lax.scan(sweep, restrict(starts[0]), change[:-1])
    return jnp.concatenate([starts[:1], corrected], axis=0)
```

```python
import functools

import jax
import jax.numpy as jnp
from jax import lax
from jax.experimental import pallas as pl
from jax.experimental.pallas import tpu as pltpu
from jax.sharding import PartitionSpec as P

FSTEPS = 16
CSTEPS = 2

fine_rate = 0.08
fine_advect = 0.04
coarse_rate = 0.16
coarse_advect = 0.16

PAD = 8
MESH = pl.DeviceIdType.MESH


def step(src, dst, layer, rows, rate, advect, shift):
    lanes = src.shape[-1]
    lane = lax.broadcasted_iota(jnp.int32, (8, lanes), 1)
    first, last = lane < shift, lane >= lanes - shift
    for row in range(rows[0], rows[1], 8):
        here = [src[layer, c, pl.ds(row, 8), :] for c in range(3)]
        ax, ay, az = (advect * v for v in here)
        xp, xm = rate - ax, rate + ax
        yp, ym = rate - ay, rate + ay
        zp = jnp.where(last, 0.0, rate - az)
        zm = jnp.where(first, 0.0, rate + az)
        for c in range(3):
            x_part = xp * src[layer + 1, c, pl.ds(row, 8), :] + xm * src[layer - 1, c, pl.ds(row, 8), :]
            y_part = yp * src[layer, c, pl.ds(row + 1, 8), :] + ym * src[layer, c, pl.ds(row - 1, 8), :]
            z_part = zp * pltpu.roll(here[c], lanes - shift, 1) + zm * pltpu.roll(here[c], shift, 1)
            dst[layer, c, pl.ds(row, 8), :] = (1.0 - 6.0 * rate) * here[c] + x_part + (y_part + z_part)


def kernel(S, N, x_ref, out_ref, state, level, ca, cb, old, adv, pk_old, pk_rch, pk_cs, rc_old, rc_rch, rc_cs,
           chg, rc_chg, spread, halo_send, halo_recv, small_send, small_recv, cs_send, cs_recv, chg_send, chg_recv):
    n, s = lax.axis_index("cuts"), lax.axis_index("space")
    W, NY, NZ = x_ref.shape[2], x_ref.shape[3], x_ref.shape[4]
    CW, CY = W // 2, NY // 2
    rounds = FSTEPS // W
    has_left, has_right = s > 0, s < S - 1
    before, after, following = lax.rem(s + S - 1, S), lax.rem(s + 1, S), lax.rem(n + 1, N)

    pairs = [(n, s - 1), (n, s + 1)]
    for d in (-1, 0, 1):
        pairs += [(n + 1, s + d), (n - 1, s + d)]
    conds = [(i >= 0) & (i < N) & (j >= 0) & (j < S) for i, j in pairs]
    if N > 2:
        for d in (-1, 0, 1):
            pairs += [(n + 2, s + d), (n - 2, s + d)]
            conds += [(n == 0) & (s + d >= 0) & (s + d < S), (n == 2) & (s + d >= 0) & (s + d < S)]
    barrier = pltpu.get_barrier_semaphore()
    count = 0
    for (i, j), cond in zip(pairs, conds):
        @pl.when(cond)
        def _():
            pl.semaphore_signal(barrier, inc=1, device_id=(i, j), device_id_type=MESH)
        count = count + jnp.where(cond, 1, 0)

    zero = jnp.zeros((PAD, NZ), jnp.float32)

    def clear(layer, _):
        for c in range(3):
            for top in (0, PAD + NY):
                for k in range(2):
                    state[k, layer, c, pl.ds(top, PAD), :] = zero
                for k in range(W - 1):
                    level[k, layer, c, pl.ds(top, PAD), :] = zero
        return 0

    def clear_halo(layer, _):
        for c in range(3):
            for row in range(PAD, PAD + NY, 8):
                for k in range(2):
                    state[k, layer, c, pl.ds(row, 8), :] = zero
                for k in range(W - 1):
                    level[k, layer, c, pl.ds(row, 8), :] = zero
        return 0

    lax.fori_loop(0, 3 * W, clear, 0)
    lax.fori_loop(jnp.where(has_left, W, 0), W, clear_halo, 0)
    lax.fori_loop(2 * W, jnp.where(has_right, 2 * W, 3 * W), clear_halo, 0)
    for i in range(3 * CW):
        for c in range(3):
            for row in range(0, CY + 2 * PAD, 8):
                if row < PAD or row >= PAD + CY:
                    ca[i, c, pl.ds(row, 8), :] = zero
                cb[i, c, pl.ds(row, 8), :] = zero
    for k in (0, 2):
        @pl.when(jnp.logical_not(has_left if k == 0 else has_right))
        def _():
            rc_cs[k] = jnp.zeros_like(rc_cs[k])
    for i in range(W):
        for c in range(3):
            state[0, W + i, c, pl.ds(PAD, NY), :] = x_ref[0, c, i]
    pl.semaphore_wait(barrier, count)

    inner = pl.ds(PAD, NY)

    def to_right(slot):
        return pltpu.make_async_remote_copy(
            src_ref=state.at[slot, pl.ds(W, W), :, inner], dst_ref=state.at[slot, pl.ds(0, W), :, inner],
            send_sem=halo_send.at[slot, 0], recv_sem=halo_recv.at[slot, 0], device_id=(n, after), device_id_type=MESH)

    def to_left(slot):
        return pltpu.make_async_remote_copy(
            src_ref=state.at[slot, pl.ds(W, W), :, inner], dst_ref=state.at[slot, pl.ds(2 * W, W), :, inner],
            send_sem=halo_send.at[slot, 1], recv_sem=halo_recv.at[slot, 1], device_id=(n, before), device_id_type=MESH)

    def send_halo(slot):
        @pl.when(has_right)
        def _():
            to_right(slot).start()

        @pl.when(has_left)
        def _():
            to_left(slot).start()

    def receive_halo(slot):
        @pl.when(has_left)
        def _():
            to_right(slot).wait_recv()

        @pl.when(has_right)
        def _():
            to_left(slot).wait_recv()

    def sent_halo(slot):
        @pl.when(has_right)
        def _():
            to_right(slot).wait_send()

        @pl.when(has_left)
        def _():
            to_left(slot).wait_send()

    even = lax.broadcasted_iota(jnp.int32, (CY, NZ), 1) % 2 == 0

    def restricted(read):
        total = (read(0, 0) + read(0, 1)) + (read(1, 0) + read(1, 1))
        other = jnp.where(even, pltpu.roll(total, NZ - 1, 1), pltpu.roll(total, 1, 1))
        return (total + other) * 0.125

    def packed(a, b):
        return jnp.where(even, a, b)

    def unpacked(v):
        return jnp.where(even, v, pltpu.roll(v, 1, 1)), jnp.where(even, pltpu.roll(v, NZ - 1, 1), v)

    def coarse_run(dest):
        lo = jnp.where(has_left, 1, CW)
        hi = jnp.where(has_right, 3 * CW - 1, 2 * CW)

        def one(i, _):
            step(ca, cb, i, (PAD, PAD + CY), coarse_rate, coarse_advect, 2)
            return 0

        def two(i, _):
            step(cb, dest, i, (PAD, PAD + CY), coarse_rate, coarse_advect, 2)
            return 0

        lax.fori_loop(lo, hi, one, 0)
        lax.fori_loop(CW, 2 * CW, two, 0)

    def small(k, src, dst, target):
        return pltpu.make_async_remote_copy(
            src_ref=src, dst_ref=dst, send_sem=small_send.at[k], recv_sem=small_recv.at[k],
            device_id=target, device_id_type=MESH)

    crow = pl.ds(PAD, CY)
    send_old = small(0, pk_old, rc_old, (following, s))
    send_rch = small(1, pk_rch, rc_rch, (following, s))

    send_halo(0)
    receive_halo(0)

    def restrict_layer(i, _):
        for c in range(3):
            ca[i, c, crow, :] = restricted(lambda l, r: state[0, 2 * i + l, c, pl.ds(PAD + r, CY, stride=2), :])
        return 0

    lax.fori_loop(0, 3 * CW, restrict_layer, 0)

    def one_round(r, _):
        slot = lax.rem(r, 2)
        for k in range(1, W + 1):
            src = state.at[slot] if k == 1 else level.at[k - 2]
            dst = state.at[1 - slot] if k == W else level.at[k - 1]
            lo = jnp.where(has_left, k, W)
            hi = jnp.where(has_right, 3 * W - k, 2 * W)

            def layer(i, _):
                step(src, dst, i, (PAD, PAD + NY), fine_rate, fine_advect, 1)
                return 0

            lax.fori_loop(lo, hi, layer, 0)
        sent_halo(slot)

        @pl.when(r < rounds - 1)
        def _():
            send_halo(1 - slot)

        @pl.when(r == 0)
        def _():
            coarse_run(old)

            @pl.when(n == 0)
            def _():
                for c in range(3):
                    pk_old[c] = packed(old[CW, c, crow, :], old[CW + 1, c, crow, :])
                send_old.start()

        @pl.when(r < rounds - 1)
        def _():
            receive_halo(1 - slot)
        return 0

    lax.fori_loop(0, rounds, one_round, 0)
    end = rounds % 2

    for i in range(CW):
        for c in range(3):
            base = old[CW + i, c, crow, :]
            for l in range(2):
                for r in range(2):
                    chg[2 * i + l, c, pl.ds(r, CY, stride=2), :] = (
                        state[end, W + 2 * i + l, c, pl.ds(PAD + r, CY, stride=2), :] - base)
    for c in range(3):
        rch = [restricted(lambda l, r: chg[2 * i + l, c, pl.ds(r, CY, stride=2), :]) for i in range(CW)]
        pk_rch[c] = packed(*rch)
        pk_cs[c] = packed(*(rch[i] + old[CW + i, c, crow, :] for i in range(CW)))

    def to_state(d, group):
        return pltpu.make_async_remote_copy(
            src_ref=pk_cs, dst_ref=rc_cs.at[1 - d], send_sem=cs_send.at[1 - d], recv_sem=cs_recv.at[1 - d],
            device_id=(group, lax.rem(s + d + S, S)), device_id_type=MESH)

    def each_target(do):
        for d in (0, 1, -1):
            @pl.when((s + d >= 0) & (s + d < S))
            def _():
                do(d)

    send_chg = pltpu.make_async_remote_copy(
        src_ref=chg.at[:, :, pl.ds(0, NY)], dst_ref=rc_chg, send_sem=chg_send, recv_sem=chg_recv, device_id=(following, s), device_id_type=MESH)

    if N > 2:
        @pl.when(n == 0)
        def _():
            each_target(lambda d: to_state(d, 2).start())

        @pl.when((n >= 1) & (n <= N - 3))
        def _():
            send_rch.start()

    @pl.when(n < N - 1)
    def _():
        send_chg.start()

    @pl.when(n == 1)
    def _():
        send_old.wait_recv()
        for c in range(3):
            for i, v in enumerate(unpacked(rc_old[c])):
                adv[CW + i, c, crow, :] = v

    if N > 2:
        @pl.when(n == 0)
        def _():
            each_target(lambda d: to_state(d, 2).wait_send())

        @pl.when((n >= 1) & (n <= N - 3))
        def _():
            send_rch.wait_send()

        @pl.when(n >= 2)
        def _():
            each_target(lambda d: to_state(-d, n).wait_recv())
            for k in range(3):
                for c in range(3):
                    for i, v in enumerate(unpacked(rc_cs[k, c])):
                        ca[k * CW + i, c, crow, :] = v
            coarse_run(adv)

            @pl.when(n <= N - 2)
            def _():
                send_rch.wait_recv()
                for c in range(3):
                    rch = unpacked(rc_rch[c])
                    pk_cs[c] = packed(*(adv[CW + i, c, crow, :] + rch[i] for i in range(CW)))
                each_target(lambda d: to_state(d, following).start())
                each_target(lambda d: to_state(d, following).wait_send())

    @pl.when(n == 0)
    def _():
        send_old.wait_send()
        out_ref[...] = x_ref[...]

    @pl.when(n > 0)
    def _():
        send_chg.wait_recv()
        for i in range(CW):
            for c in range(3):
                base = adv[CW + i, c, crow, :]
                for r in range(2):
                    spread[i, c, pl.ds(r, CY, stride=2), :] = base
        for i in range(W):
            for c in range(3):
                out_ref[0, c, i] = spread[i // 2, c, pl.ds(0, NY), :] + rc_chg[i, c]

    @pl.when(n < N - 1)
    def _():
        send_chg.wait_send()


def shards(S, N, starts):
    W, NY, NZ = starts.shape[2:]
    assert W == 4 and FSTEPS % W == 0 and CSTEPS == 2
    f32 = jnp.float32
    CW, CY = W // 2, NY // 2
    packed = pltpu.VMEM((3, CY, NZ), f32)
    coarse = pltpu.VMEM((3 * CW, 3, CY + 2 * PAD, NZ), f32)
    dma = pltpu.SemaphoreType.DMA
    return pl.pallas_call(
        functools.partial(kernel, S, N),
        out_shape=jax.ShapeDtypeStruct(starts.shape, f32),
        in_specs=[pl.BlockSpec(memory_space=pltpu.VMEM)],
        out_specs=pl.BlockSpec(memory_space=pltpu.VMEM),
        scratch_shapes=[
            pltpu.VMEM((2, 3 * W, 3, NY + 2 * PAD, NZ), f32),
            pltpu.VMEM((W - 1, 3 * W, 3, NY + 2 * PAD, NZ), f32),
            coarse, coarse, coarse, coarse,
            packed, packed, packed, packed, packed,
            pltpu.VMEM((3, 3, CY, NZ), f32),
            pltpu.VMEM((W, 3, NY + PAD, NZ), f32),
            pltpu.VMEM((W, 3, NY, NZ), f32),
            pltpu.VMEM((CW, 3, NY + PAD, NZ), f32),
            dma((2, 2)), dma((2, 2)), dma((2,)), dma((2,)), dma((3,)), dma((3,)), dma, dma,
        ],
        compiler_params=pltpu.CompilerParams(collective_id=0, has_side_effects=True),
    )(starts)


def solution(mesh):
    placed = P("cuts", None, "space", None, None)
    return jax.shard_map(
        functools.partial(shards, mesh.shape["space"], mesh.shape["cuts"]),
        mesh=mesh, in_specs=(placed,), out_specs=placed, check_vma=False)
```

```python
import functools

import jax
import jax.numpy as jnp
from jax import lax
from jax.experimental import pallas as pl
from jax.experimental.pallas import tpu as pltpu
from jax.sharding import PartitionSpec as P

FSTEPS = 16
CSTEPS = 2

fine_rate = 0.08
fine_advect = 0.04
coarse_rate = 0.16
coarse_advect = 0.16

PAD = 8
MESH = pl.DeviceIdType.MESH


def step(src, dst, layers, tiles, rate, advect, shift):
    lanes = src.shape[-1]
    lane = lax.broadcasted_iota(jnp.int32, (8, lanes), 1)
    first, last = lane < shift, lane >= lanes - shift
    for row in tiles:
        for layer, keep in layers:
            here = [src[layer, c, pl.ds(row, 8), :] for c in range(3)]
            ax, ay, az = (advect * v for v in here)
            xp, xm = rate - ax, rate + ax
            yp, ym = rate - ay, rate + ay
            zp = jnp.where(last, 0.0, rate - az)
            zm = jnp.where(first, 0.0, rate + az)
            for c in range(3):
                x_part = xp * src[layer + 1, c, pl.ds(row, 8), :] + xm * src[layer - 1, c, pl.ds(row, 8), :]
                y_part = yp * src[layer, c, pl.ds(row + 1, 8), :] + ym * src[layer, c, pl.ds(row - 1, 8), :]
                z_part = zp * pltpu.roll(here[c], lanes - shift, 1) + zm * pltpu.roll(here[c], shift, 1)
                new = (1.0 - 6.0 * rate) * here[c] + x_part + (y_part + z_part)
                dst[layer, c, pl.ds(row, 8), :] = new if keep is None else jnp.where(keep, new, 0.0)


def kernel(S, N, x_ref, out_ref, state, level, ca, cb, old, adv, pk_old, pk_rch, pk_cs, rc_old, rc_rch, rc_cs,
           chg, rc_chg, spread, halo_send, halo_recv, small_send, small_recv, cs_send, cs_recv, chg_send, chg_recv):
    n, s = lax.axis_index("cuts"), lax.axis_index("space")
    W, NY, NZ = x_ref.shape[2], x_ref.shape[3], x_ref.shape[4]
    CW, CY = W // 2, NY // 2
    rounds = FSTEPS // W
    has_left, has_right = s > 0, s < S - 1
    before, after, following = lax.rem(s + S - 1, S), lax.rem(s + 1, S), lax.rem(n + 1, N)

    pairs = [(n, s - 1), (n, s + 1)]
    for d in (-1, 0, 1):
        pairs += [(n + 1, s + d), (n - 1, s + d)]
    conds = [(i >= 0) & (i < N) & (j >= 0) & (j < S) for i, j in pairs]
    if N > 2:
        for d in (-1, 0, 1):
            pairs += [(n + 2, s + d), (n - 2, s + d)]
            conds += [(n == 0) & (s + d >= 0) & (s + d < S), (n == 2) & (s + d >= 0) & (s + d < S)]
    barrier = pltpu.get_barrier_semaphore()
    count = 0
    for (i, j), cond in zip(pairs, conds):
        @pl.when(cond)
        def _():
            pl.semaphore_signal(barrier, inc=1, device_id=(i, j), device_id_type=MESH)
        count = count + jnp.where(cond, 1, 0)

    zero = jnp.zeros((PAD, NZ), jnp.float32)

    def clear(layer, _):
        for c in range(3):
            for top in (0, PAD + NY):
                for k in range(2):
                    state[k, layer, c, pl.ds(top, PAD), :] = zero
                for k in range(W - 1):
                    level[k, layer, c, pl.ds(top, PAD), :] = zero
        return 0

    def clear_halo(layer, _):
        for c in range(3):
            for row in range(PAD, PAD + NY, 8):
                for k in range(2):
                    state[k, layer, c, pl.ds(row, 8), :] = zero
                for k in range(W - 1):
                    level[k, layer, c, pl.ds(row, 8), :] = zero
        return 0

    lax.fori_loop(0, 3 * W, clear, 0)
    lax.fori_loop(jnp.where(has_left, W, 0), W, clear_halo, 0)
    lax.fori_loop(2 * W, jnp.where(has_right, 2 * W, 3 * W), clear_halo, 0)
    for i in range(3 * CW):
        for c in range(3):
            for row in range(0, CY + 2 * PAD, 8):
                if row < PAD or row >= PAD + CY:
                    ca[i, c, pl.ds(row, 8), :] = zero
                cb[i, c, pl.ds(row, 8), :] = zero
    for k in (0, 2):
        @pl.when(jnp.logical_not(has_left if k == 0 else has_right))
        def _():
            rc_cs[k] = jnp.zeros_like(rc_cs[k])
    for i in range(W):
        for c in range(3):
            state[0, W + i, c, pl.ds(PAD, NY), :] = x_ref[0, c, i]
    pl.semaphore_wait(barrier, count)

    half = (NY // 8 + rounds) // 2 * 8
    bounds = [half - 8 * r for r in range(rounds + 1)]
    assert 8 <= bounds[-1] and bounds[0] < NY

    def rows_of(r, piece):
        return pl.ds(PAD, bounds[r]) if piece == 0 else pl.ds(PAD + bounds[r], NY - bounds[r])

    def to_right(r, piece):
        slot, rows = r % 2, rows_of(r, piece)
        return pltpu.make_async_remote_copy(
            src_ref=state.at[slot, pl.ds(W, W), :, rows], dst_ref=state.at[slot, pl.ds(0, W), :, rows],
            send_sem=halo_send.at[slot, 0, piece], recv_sem=halo_recv.at[slot, 0, piece],
            device_id=(n, after), device_id_type=MESH)

    def to_left(r, piece):
        slot, rows = r % 2, rows_of(r, piece)
        return pltpu.make_async_remote_copy(
            src_ref=state.at[slot, pl.ds(W, W), :, rows], dst_ref=state.at[slot, pl.ds(2 * W, W), :, rows],
            send_sem=halo_send.at[slot, 1, piece], recv_sem=halo_recv.at[slot, 1, piece],
            device_id=(n, before), device_id_type=MESH)

    def send_halo(r, piece):
        @pl.when(has_right)
        def _():
            to_right(r, piece).start()

        @pl.when(has_left)
        def _():
            to_left(r, piece).start()

    def receive_halo(r, piece):
        @pl.when(has_left)
        def _():
            to_right(r, piece).wait_recv()

        @pl.when(has_right)
        def _():
            to_left(r, piece).wait_recv()

    def sent_halo(r):
        for piece in range(2):
            @pl.when(has_right)
            def _():
                to_right(r, piece).wait_send()

            @pl.when(has_left)
            def _():
                to_left(r, piece).wait_send()

    even = lax.broadcasted_iota(jnp.int32, (CY, NZ), 1) % 2 == 0

    def restricted(read):
        total = (read(0, 0) + read(0, 1)) + (read(1, 0) + read(1, 1))
        even = lax.broadcasted_iota(jnp.int32, total.shape, 1) % 2 == 0
        other = jnp.where(even, pltpu.roll(total, NZ - 1, 1), pltpu.roll(total, 1, 1))
        return (total + other) * 0.125

    def packed(a, b):
        return jnp.where(even, a, b)

    def unpacked(v):
        return jnp.where(even, v, pltpu.roll(v, 1, 1)), jnp.where(even, pltpu.roll(v, NZ - 1, 1), v)

    def coarse_run(dest):
        tiles = range(PAD, PAD + CY, 8)
        for i in range(1, CW + CW // 2):
            keep = (has_left, has_right) if i < CW else (None, None)
            step(ca, cb, ((i, keep[0]), (3 * CW - 1 - i, keep[1])), tiles, coarse_rate, coarse_advect, 2)
        for i in range(CW, CW + CW // 2):
            step(cb, dest, ((i, None), (3 * CW - 1 - i, None)), tiles, coarse_rate, coarse_advect, 2)

    def small(k, src, dst, target):
        return pltpu.make_async_remote_copy(
            src_ref=src, dst_ref=dst, send_sem=small_send.at[k], recv_sem=small_recv.at[k],
            device_id=target, device_id_type=MESH)

    crow = pl.ds(PAD, CY)
    send_old = small(0, pk_old, rc_old, (following, s))
    send_rch = small(1, pk_rch, rc_rch, (following, s))

    def fine_piece(r, piece):
        bound = PAD + bounds[r]
        for k in range(1, W + 1):
            src = state.at[r % 2] if k == 1 else level.at[k - 2]
            dst = state.at[(r + 1) % 2] if k == W else level.at[k - 1]
            if piece == 0:
                tiles = list(range(PAD, bound - 8, 8)) + [bound - 8 - k]
            else:
                tiles = [bound - k] + list(range(bound, PAD + NY, 8))
            if k == W and piece == 0 and r > 0:
                sent_halo(r - 1)

            def pair(i, _):
                step(src, dst, ((i, has_left | (i >= W)), (3 * W - 1 - i, has_right | (i >= W))), tiles,
                     fine_rate, fine_advect, 1)
                return 0

            lax.fori_loop(k, W + W // 2, pair, 0)

    def restrict_piece(piece):
        first, last = (0, bounds[0] // 2) if piece == 0 else (bounds[0] // 2, CY)

        def restrict_layer(i, _):
            for c in range(3):
                ca[i, c, pl.ds(PAD + first, last - first), :] = restricted(
                    lambda l, r: state[0, 2 * i + l, c, pl.ds(PAD + 2 * first + r, last - first, stride=2), :])
            return 0

        lax.fori_loop(0, 3 * CW, restrict_layer, 0)

    for piece in range(2):
        send_halo(0, piece)
    for r in range(rounds):
        for piece in range(2):
            receive_halo(r, piece)
            if r == 0:
                restrict_piece(piece)
            fine_piece(r, piece)
            if r < rounds - 1:
                send_halo(r + 1, piece)
        if r == 0:
            coarse_run(old)

            @pl.when(n == 0)
            def _():
                for c in range(3):
                    pk_old[c] = packed(old[CW, c, crow, :], old[CW + 1, c, crow, :])
                send_old.start()
    sent_halo(rounds - 1)
    end = rounds % 2

    for i in range(CW):
        for c in range(3):
            base = old[CW + i, c, crow, :]
            for l in range(2):
                for r in range(2):
                    chg[2 * i + l, c, pl.ds(r, CY, stride=2), :] = (
                        state[end, W + 2 * i + l, c, pl.ds(PAD + r, CY, stride=2), :] - base)
    for c in range(3):
        rch = [restricted(lambda l, r: chg[2 * i + l, c, pl.ds(r, CY, stride=2), :]) for i in range(CW)]
        pk_rch[c] = packed(*rch)
        pk_cs[c] = packed(*(rch[i] + old[CW + i, c, crow, :] for i in range(CW)))

    def to_state(d, group):
        return pltpu.make_async_remote_copy(
            src_ref=pk_cs, dst_ref=rc_cs.at[1 - d], send_sem=cs_send.at[1 - d], recv_sem=cs_recv.at[1 - d],
            device_id=(group, lax.rem(s + d + S, S)), device_id_type=MESH)

    def each_target(do):
        for d in (0, 1, -1):
            @pl.when((s + d >= 0) & (s + d < S))
            def _():
                do(d)

    send_chg = pltpu.make_async_remote_copy(
        src_ref=chg.at[:, :, pl.ds(0, NY)], dst_ref=rc_chg, send_sem=chg_send, recv_sem=chg_recv, device_id=(following, s), device_id_type=MESH)

    if N > 2:
        @pl.when(n == 0)
        def _():
            each_target(lambda d: to_state(d, 2).start())

        @pl.when((n >= 1) & (n <= N - 3))
        def _():
            send_rch.start()

    @pl.when(n < N - 1)
    def _():
        send_chg.start()

    @pl.when(n == 1)
    def _():
        send_old.wait_recv()
        for c in range(3):
            for i, v in enumerate(unpacked(rc_old[c])):
                adv[CW + i, c, crow, :] = v

    if N > 2:
        @pl.when(n == 0)
        def _():
            each_target(lambda d: to_state(d, 2).wait_send())

        @pl.when((n >= 1) & (n <= N - 3))
        def _():
            send_rch.wait_send()

        @pl.when(n >= 2)
        def _():
            each_target(lambda d: to_state(-d, n).wait_recv())
            for k in range(3):
                for c in range(3):
                    for i, v in enumerate(unpacked(rc_cs[k, c])):
                        ca[k * CW + i, c, crow, :] = v
            coarse_run(adv)

            @pl.when(n <= N - 2)
            def _():
                send_rch.wait_recv()
                for c in range(3):
                    rch = unpacked(rc_rch[c])
                    pk_cs[c] = packed(*(adv[CW + i, c, crow, :] + rch[i] for i in range(CW)))
                each_target(lambda d: to_state(d, following).start())
                each_target(lambda d: to_state(d, following).wait_send())

    @pl.when(n == 0)
    def _():
        send_old.wait_send()
        out_ref[...] = x_ref[...]

    @pl.when(n > 0)
    def _():
        send_chg.wait_recv()
        for i in range(CW):
            for c in range(3):
                base = adv[CW + i, c, crow, :]
                for r in range(2):
                    spread[i, c, pl.ds(r, CY, stride=2), :] = base
        for i in range(W):
            for c in range(3):
                out_ref[0, c, i] = spread[i // 2, c, pl.ds(0, NY), :] + rc_chg[i, c]

    @pl.when(n < N - 1)
    def _():
        send_chg.wait_send()


def shards(S, N, starts):
    W, NY, NZ = starts.shape[2:]
    assert W == 4 and FSTEPS % W == 0 and CSTEPS == 2
    f32 = jnp.float32
    CW, CY = W // 2, NY // 2
    packed = pltpu.VMEM((3, CY, NZ), f32)
    coarse = pltpu.VMEM((3 * CW, 3, CY + 2 * PAD, NZ), f32)
    dma = pltpu.SemaphoreType.DMA
    return pl.pallas_call(
        functools.partial(kernel, S, N),
        out_shape=jax.ShapeDtypeStruct(starts.shape, f32),
        in_specs=[pl.BlockSpec(memory_space=pltpu.VMEM)],
        out_specs=pl.BlockSpec(memory_space=pltpu.VMEM),
        scratch_shapes=[
            pltpu.VMEM((2, 3 * W, 3, NY + 2 * PAD, NZ), f32),
            pltpu.VMEM((W - 1, 3 * W, 3, NY + 2 * PAD, NZ), f32),
            coarse, coarse, coarse, coarse,
            packed, packed, packed, packed, packed,
            pltpu.VMEM((3, 3, CY, NZ), f32),
            pltpu.VMEM((W, 3, NY + PAD, NZ), f32),
            pltpu.VMEM((W, 3, NY, NZ), f32),
            pltpu.VMEM((CW, 3, NY + PAD, NZ), f32),
            dma((2, 2, 2)), dma((2, 2, 2)), dma((2,)), dma((2,)), dma((3,)), dma((3,)), dma, dma,
        ],
        compiler_params=pltpu.CompilerParams(collective_id=0, has_side_effects=True),
    )(starts)


def solution(mesh):
    placed = P("cuts", None, "space", None, None)
    return jax.shard_map(
        functools.partial(shards, mesh.shape["space"], mesh.shape["cuts"]),
        mesh=mesh, in_specs=(placed,), out_specs=placed, check_vma=False)
```

```python
import functools

import jax
import jax.numpy as jnp
from jax import lax
from jax.experimental import pallas as pl
from jax.experimental.pallas import tpu as pltpu
from jax.sharding import PartitionSpec as P

FSTEPS = 16
CSTEPS = 2

fine_rate = 0.08
fine_advect = 0.04
coarse_rate = 0.16
coarse_advect = 0.16

PAD = 8
MESH = pl.DeviceIdType.MESH


GROUP = 8


def step(src, dst, layers, rows, rate, advect, shift):
    lanes = src.shape[-1]
    lane = lax.broadcasted_iota(jnp.int32, (8, lanes), 1)
    first, last = lane < shift, lane >= lanes - shift
    items = [(layer, keep, row) for row in range(rows[0], rows[1], 8) for layer, keep in layers]
    groups = [items[i:i + GROUP] for i in range(0, len(items), GROUP)]

    def shifted(group):
        here = [[src[layer, c, pl.ds(row, 8), :] for c in range(3)] for layer, keep, row in group]
        return [[(v, pltpu.roll(v, lanes - shift, 1), pltpu.roll(v, shift, 1)) for v in vs] for vs in here]

    ready = shifted(groups[0])
    for g, group in enumerate(groups):
        values, ready = ready, shifted(groups[g + 1]) if g + 1 < len(groups) else None
        new = []
        for (layer, keep, row), vs in zip(group, values):
            ax, ay, az = (advect * v[0] for v in vs)
            xp, xm = rate - ax, rate + ax
            yp, ym = rate - ay, rate + ay
            zp = jnp.where(last, 0.0, rate - az)
            zm = jnp.where(first, 0.0, rate + az)
            for c in range(3):
                x_part = xp * src[layer + 1, c, pl.ds(row, 8), :] + xm * src[layer - 1, c, pl.ds(row, 8), :]
                y_part = yp * src[layer, c, pl.ds(row + 1, 8), :] + ym * src[layer, c, pl.ds(row - 1, 8), :]
                z_part = zp * vs[c][1] + zm * vs[c][2]
                value = ((1.0 - 6.0 * rate) * vs[c][0] + x_part) + (y_part + z_part)
                new.append(value if keep is None else jnp.where(keep, value, 0.0))
        for j, (layer, keep, row) in enumerate(group):
            for c in range(3):
                dst[layer, c, pl.ds(row, 8), :] = new[3 * j + c]


def kernel(S, N, x_ref, out_ref, state, level, ca, cb, old, adv, pk_old, pk_rch, pk_cs, rc_old, rc_rch, rc_cs,
           chg, rc_chg, spread, halo_send, halo_recv, small_send, small_recv, cs_send, cs_recv, chg_send, chg_recv):
    n, s = lax.axis_index("cuts"), lax.axis_index("space")
    W, NY, NZ = x_ref.shape[2], x_ref.shape[3], x_ref.shape[4]
    CW, CY = W // 2, NY // 2
    rounds = FSTEPS // W
    has_left, has_right = s > 0, s < S - 1
    before, after, following = lax.rem(s + S - 1, S), lax.rem(s + 1, S), lax.rem(n + 1, N)

    pairs = [(n, s - 1), (n, s + 1)]
    for d in (-1, 0, 1):
        pairs += [(n + 1, s + d), (n - 1, s + d)]
    conds = [(i >= 0) & (i < N) & (j >= 0) & (j < S) for i, j in pairs]
    if N > 2:
        for d in (-1, 0, 1):
            pairs += [(n + 2, s + d), (n - 2, s + d)]
            conds += [(n == 0) & (s + d >= 0) & (s + d < S), (n == 2) & (s + d >= 0) & (s + d < S)]
    barrier = pltpu.get_barrier_semaphore()
    count = 0
    for (i, j), cond in zip(pairs, conds):
        @pl.when(cond)
        def _():
            pl.semaphore_signal(barrier, inc=1, device_id=(i, j), device_id_type=MESH)
        count = count + jnp.where(cond, 1, 0)

    zero = jnp.zeros((PAD, NZ), jnp.float32)

    def clear(layer, _):
        for c in range(3):
            for top in (0, PAD + NY):
                for k in range(2):
                    state[k, layer, c, pl.ds(top, PAD), :] = zero
                for k in range(W - 1):
                    level[k, layer, c, pl.ds(top, PAD), :] = zero
        return 0

    def clear_halo(layer, _):
        for c in range(3):
            for row in range(PAD, PAD + NY, 8):
                for k in range(2):
                    state[k, layer, c, pl.ds(row, 8), :] = zero
                for k in range(W - 1):
                    level[k, layer, c, pl.ds(row, 8), :] = zero
        return 0

    lax.fori_loop(0, 3 * W, clear, 0)
    lax.fori_loop(jnp.where(has_left, W, 0), W, clear_halo, 0)
    lax.fori_loop(2 * W, jnp.where(has_right, 2 * W, 3 * W), clear_halo, 0)
    for i in range(3 * CW):
        for c in range(3):
            for row in range(0, CY + 2 * PAD, 8):
                if row < PAD or row >= PAD + CY:
                    ca[i, c, pl.ds(row, 8), :] = zero
                cb[i, c, pl.ds(row, 8), :] = zero
    for k in (0, 2):
        @pl.when(jnp.logical_not(has_left if k == 0 else has_right))
        def _():
            rc_cs[k] = jnp.zeros_like(rc_cs[k])
    for i in range(W):
        for c in range(3):
            state[0, W + i, c, pl.ds(PAD, NY), :] = x_ref[0, c, i]
    pl.semaphore_wait(barrier, count)

    inner = pl.ds(PAD, NY)

    def to_right(slot):
        return pltpu.make_async_remote_copy(
            src_ref=state.at[slot, pl.ds(W, W), :, inner], dst_ref=state.at[slot, pl.ds(0, W), :, inner],
            send_sem=halo_send.at[slot, 0], recv_sem=halo_recv.at[slot, 0], device_id=(n, after), device_id_type=MESH)

    def to_left(slot):
        return pltpu.make_async_remote_copy(
            src_ref=state.at[slot, pl.ds(W, W), :, inner], dst_ref=state.at[slot, pl.ds(2 * W, W), :, inner],
            send_sem=halo_send.at[slot, 1], recv_sem=halo_recv.at[slot, 1], device_id=(n, before), device_id_type=MESH)

    def send_halo(slot):
        @pl.when(has_right)
        def _():
            to_right(slot).start()

        @pl.when(has_left)
        def _():
            to_left(slot).start()

    def receive_halo(slot):
        @pl.when(has_left)
        def _():
            to_right(slot).wait_recv()

        @pl.when(has_right)
        def _():
            to_left(slot).wait_recv()

    def sent_halo(slot):
        @pl.when(has_right)
        def _():
            to_right(slot).wait_send()

        @pl.when(has_left)
        def _():
            to_left(slot).wait_send()

    even = lax.broadcasted_iota(jnp.int32, (CY, NZ), 1) % 2 == 0

    def restricted(read):
        total = (read(0, 0) + read(0, 1)) + (read(1, 0) + read(1, 1))
        other = jnp.where(even, pltpu.roll(total, NZ - 1, 1), pltpu.roll(total, 1, 1))
        return (total + other) * 0.125

    def packed(a, b):
        return jnp.where(even, a, b)

    def unpacked(v):
        return jnp.where(even, v, pltpu.roll(v, 1, 1)), jnp.where(even, pltpu.roll(v, NZ - 1, 1), v)

    def coarse_run(dest):
        rows = (PAD, PAD + CY)
        for i in range(1, CW + CW // 2):
            keep = (has_left, has_right) if i < CW else (None, None)
            step(ca, cb, ((i, keep[0]), (3 * CW - 1 - i, keep[1])), rows, coarse_rate, coarse_advect, 2)
        for i in range(CW, CW + CW // 2):
            step(cb, dest, ((i, None), (3 * CW - 1 - i, None)), rows, coarse_rate, coarse_advect, 2)

    def small(k, src, dst, target):
        return pltpu.make_async_remote_copy(
            src_ref=src, dst_ref=dst, send_sem=small_send.at[k], recv_sem=small_recv.at[k],
            device_id=target, device_id_type=MESH)

    crow = pl.ds(PAD, CY)
    send_old = small(0, pk_old, rc_old, (following, s))
    send_rch = small(1, pk_rch, rc_rch, (following, s))

    send_halo(0)
    receive_halo(0)

    def restrict_layer(i, _):
        for c in range(3):
            ca[i, c, crow, :] = restricted(lambda l, r: state[0, 2 * i + l, c, pl.ds(PAD + r, CY, stride=2), :])
        return 0

    lax.fori_loop(0, 3 * CW, restrict_layer, 0)

    def one_round(r, _):
        slot = lax.rem(r, 2)
        for k in range(1, W + 1):
            src = state.at[slot] if k == 1 else level.at[k - 2]
            dst = state.at[1 - slot] if k == W else level.at[k - 1]

            def pair(i, _):
                step(src, dst, ((i, has_left | (i >= W)), (3 * W - 1 - i, has_right | (i >= W))),
                     (PAD, PAD + NY), fine_rate, fine_advect, 1)
                return 0

            lax.fori_loop(k, W + W // 2, pair, 0)
        sent_halo(slot)

        @pl.when(r < rounds - 1)
        def _():
            send_halo(1 - slot)

        @pl.when(r == 0)
        def _():
            coarse_run(old)

            @pl.when(n == 0)
            def _():
                for c in range(3):
                    pk_old[c] = packed(old[CW, c, crow, :], old[CW + 1, c, crow, :])
                send_old.start()

        @pl.when(r < rounds - 1)
        def _():
            receive_halo(1 - slot)
        return 0

    lax.fori_loop(0, rounds, one_round, 0)
    end = rounds % 2

    for i in range(CW):
        for c in range(3):
            base = old[CW + i, c, crow, :]
            for l in range(2):
                for r in range(2):
                    chg[2 * i + l, c, pl.ds(r, CY, stride=2), :] = (
                        state[end, W + 2 * i + l, c, pl.ds(PAD + r, CY, stride=2), :] - base)
    for c in range(3):
        rch = [restricted(lambda l, r: chg[2 * i + l, c, pl.ds(r, CY, stride=2), :]) for i in range(CW)]
        pk_rch[c] = packed(*rch)
        pk_cs[c] = packed(*(rch[i] + old[CW + i, c, crow, :] for i in range(CW)))

    def to_state(d, group):
        return pltpu.make_async_remote_copy(
            src_ref=pk_cs, dst_ref=rc_cs.at[1 - d], send_sem=cs_send.at[1 - d], recv_sem=cs_recv.at[1 - d],
            device_id=(group, lax.rem(s + d + S, S)), device_id_type=MESH)

    def each_target(do):
        for d in (0, 1, -1):
            @pl.when((s + d >= 0) & (s + d < S))
            def _():
                do(d)

    send_chg = pltpu.make_async_remote_copy(
        src_ref=chg.at[:, :, pl.ds(0, NY)], dst_ref=rc_chg, send_sem=chg_send, recv_sem=chg_recv, device_id=(following, s), device_id_type=MESH)

    if N > 2:
        @pl.when(n == 0)
        def _():
            each_target(lambda d: to_state(d, 2).start())

        @pl.when((n >= 1) & (n <= N - 3))
        def _():
            send_rch.start()

    @pl.when(n < N - 1)
    def _():
        send_chg.start()

    @pl.when(n == 1)
    def _():
        send_old.wait_recv()
        for c in range(3):
            for i, v in enumerate(unpacked(rc_old[c])):
                adv[CW + i, c, crow, :] = v

    if N > 2:
        @pl.when(n == 0)
        def _():
            each_target(lambda d: to_state(d, 2).wait_send())

        @pl.when((n >= 1) & (n <= N - 3))
        def _():
            send_rch.wait_send()

        @pl.when(n >= 2)
        def _():
            each_target(lambda d: to_state(-d, n).wait_recv())
            for k in range(3):
                for c in range(3):
                    for i, v in enumerate(unpacked(rc_cs[k, c])):
                        ca[k * CW + i, c, crow, :] = v
            coarse_run(adv)

            @pl.when(n <= N - 2)
            def _():
                send_rch.wait_recv()
                for c in range(3):
                    rch = unpacked(rc_rch[c])
                    pk_cs[c] = packed(*(adv[CW + i, c, crow, :] + rch[i] for i in range(CW)))
                each_target(lambda d: to_state(d, following).start())
                each_target(lambda d: to_state(d, following).wait_send())

    @pl.when(n == 0)
    def _():
        send_old.wait_send()
        out_ref[...] = x_ref[...]

    @pl.when(n > 0)
    def _():
        send_chg.wait_recv()
        for i in range(CW):
            for c in range(3):
                base = adv[CW + i, c, crow, :]
                for r in range(2):
                    spread[i, c, pl.ds(r, CY, stride=2), :] = base
        for i in range(W):
            for c in range(3):
                out_ref[0, c, i] = spread[i // 2, c, pl.ds(0, NY), :] + rc_chg[i, c]

    @pl.when(n < N - 1)
    def _():
        send_chg.wait_send()


def shards(S, N, starts):
    W, NY, NZ = starts.shape[2:]
    assert W == 4 and FSTEPS % W == 0 and CSTEPS == 2
    f32 = jnp.float32
    CW, CY = W // 2, NY // 2
    packed = pltpu.VMEM((3, CY, NZ), f32)
    coarse = pltpu.VMEM((3 * CW, 3, CY + 2 * PAD, NZ), f32)
    dma = pltpu.SemaphoreType.DMA
    return pl.pallas_call(
        functools.partial(kernel, S, N),
        out_shape=jax.ShapeDtypeStruct(starts.shape, f32),
        in_specs=[pl.BlockSpec(memory_space=pltpu.VMEM)],
        out_specs=pl.BlockSpec(memory_space=pltpu.VMEM),
        scratch_shapes=[
            pltpu.VMEM((2, 3 * W, 3, NY + 2 * PAD, NZ), f32),
            pltpu.VMEM((W - 1, 3 * W, 3, NY + 2 * PAD, NZ), f32),
            coarse, coarse, coarse, coarse,
            packed, packed, packed, packed, packed,
            pltpu.VMEM((3, 3, CY, NZ), f32),
            pltpu.VMEM((W, 3, NY + PAD, NZ), f32),
            pltpu.VMEM((W, 3, NY, NZ), f32),
            pltpu.VMEM((CW, 3, NY + PAD, NZ), f32),
            dma((2, 2)), dma((2, 2)), dma((2,)), dma((2,)), dma((3,)), dma((3,)), dma, dma,
        ],
        compiler_params=pltpu.CompilerParams(collective_id=0, has_side_effects=True),
    )(starts)


def solution(mesh):
    placed = P("cuts", None, "space", None, None)
    return jax.shard_map(
        functools.partial(shards, mesh.shape["space"], mesh.shape["cuts"]),
        mesh=mesh, in_specs=(placed,), out_specs=placed, check_vma=False)
```
